256 devices in a mesh: gx: 8 (over x_lo, y), gy: 16 (over z, core), row: 2 (over x_hi).
Axes of the slice: x: 4 (x_hi: 2, x_lo: 2; x = x_hi * 2 + x_lo), y: 4, z: 8, core: 2. Of those that a mesh axis runs over, the one named last changes fastest.
Arguments:
- sources: bfloat16 [8, 16, 128, 1280], P('gx', 'gy', 'row'), may hold values from -6 to 6
- scatter: bfloat16 [8, 16, 1280, 2560], P('gx', 'gy', None, 'row'), may hold values from -0.15625 to 0.15625
Outputs:
- traces: float32 [8, 16, 128, 1280], P('gx', 'gy', 'row')
The draws below stay inside these ranges and needn't reach their ends.
All inputs are finite; a program needn't handle non-finite values.
Results may differ from the reference program's by a relative error of at most 0.017.
Values may be sent and summed in bfloat16 or wider, within the bound.
No kernel may reach another device: no remote copies, remote signals or barrier semaphores. Data moves between devices by JAX's collectives and lax.ppermute only.
A program may use at most 64 MiB of HBM per device.

```python
import jax
import jax.numpy as jnp

M = 640
RHS = 128
NSX = 8
NSY = 16


def block_scale(stream_key, dims, cuts, smallest, high):
    level, own = 1.0, jax.random.fold_in(stream_key, 6)
    for dim, shards_of in cuts:
        draws = jnp.exp(jax.random.uniform(jax.random.fold_in(own, dim), (shards_of,), jnp.float32, smallest / len(cuts), high / len(cuts)))
        level = level * jnp.repeat(draws, dims[dim] // shards_of).reshape([-1 if axis == dim else 1 for axis in range(len(dims))])
    return level


def bell_draw(key, dims, width, reach, cuts=(), held_as=jnp.bfloat16):
    values = jax.random.normal(key, dims, jnp.float32) * width
    if len(cuts) > 0:
        values = block_scale(key, dims, cuts, -0.22, 0.18) * values
    return jnp.clip(values, min=-reach, max=reach).astype(held_as)


def setup_inputs(seed: int = 0) -> dict:
    splits = jax.random.split(jax.random.key(seed), 3)
    return {
        "sources": bell_draw(splits[0], (NSX, NSY, RHS, 2 * M), 1.0, 6.0, ((0, 8), (1, 16), (2, 2))),
        "scatter": bell_draw(splits[1], (NSX, NSY, 2 * M, 4 * M), (2 * M) ** -0.5, 0.15625, ((0, 8), (1, 16), (3, 2))),
    }


def reference(sources, scatter):
    east_count = sources.shape[0]
    north_count = sources.shape[1]
    count = sources.shape[2]
    modes = sources.shape[3] // 2
    zeros_face = jnp.zeros((count, modes), jnp.bfloat16)
    east_out = {}
    north_out = {}
    west_back = {}
    south_back = {}
    inflows = {}
    for east_index in range(east_count):
        for north_index in range(north_count):
            from_west = east_out[(east_index - 1, north_index)] if east_index > 0 else zeros_face
            from_south = north_out[(east_index, north_index - 1)] if north_index > 0 else zeros_face
            inflow = sources[east_index, north_index].astype(jnp.float32) + jnp.concatenate([from_west, from_south], 1).astype(jnp.float32)
            scattered = jnp.dot(inflow.astype(jnp.bfloat16), scatter[east_index, north_index], preferred_element_type=jnp.float32)
            sent = scattered.astype(jnp.bfloat16)
            east_out[(east_index, north_index)] = sent[:, :modes]
            north_out[(east_index, north_index)] = sent[:, modes:2 * modes]
            west_back[(east_index, north_index)] = sent[:, 2 * modes:3 * modes]
            south_back[(east_index, north_index)] = sent[:, 3 * modes:]
            inflows[(east_index, north_index)] = inflow
    columns = []
    for east_index in range(east_count):
        column = []
        for north_index in range(north_count):
            from_east = west_back[(east_index + 1, north_index)] if east_index + 1 < east_count else zeros_face
            from_north = south_back[(east_index, north_index + 1)] if north_index + 1 < north_count else zeros_face
            column.append(inflows[(east_index, north_index)] + jnp.concatenate([from_east, from_north], 1).astype(jnp.float32))
        columns.append(jnp.stack(column, 0))
    return jnp.stack(columns, 0)
```

```python
import functools

import jax
import jax.numpy as jnp
from jax import lax
from jax.experimental import pallas as pl
from jax.experimental.pallas import tpu as pltpu
from jax.sharding import PartitionSpec as P

AXES = ("gx", "gy", "row")
PERIOD = 15


def place(shape, cell):
    a, b, row = cell
    return (a * shape[1] + b) * shape[2] + row


def distance(shape, one, two):
    hops = abs(one[1] // 2 - two[1] // 2)
    for i, j in ((one[0] % 4, two[0] % 4), (2 * one[2] + one[0] // 4, 2 * two[2] + two[0] // 4)):
        hops += min((i - j) % 4, (j - i) % 4)
    return hops


def completed(shape, moves):
    target = dict(moves)
    received = set(target.values())
    devices = [(a, b, row) for a in range(shape[0]) for b in range(shape[1]) for row in range(shape[2])]
    for a, b, row in devices:
        if b % 2 == 0:
            chip = [(a, b, row), (a, b + 1, row)]
            for one, two in (chip, chip[::-1]):
                if one not in target and two not in received:
                    target[one] = two
                    received.add(two)
    senders = [one for one in devices if one not in target]
    receivers = [two for two in devices if two not in received]
    options = sorted((distance(shape, one, two), one, two) for one in senders for two in receivers if one != two)
    for _, one, two in options:
        if one not in target and two not in received:
            target[one] = two
            received.add(two)
    for one in senders:
        if one not in target:
            (two,) = [two for two in receivers if two not in received]
            other = next(i for i in senders if i != one and target[i] != one)
            target[one], target[other] = target[other], two
            received.add(two)
    return [(place(shape, one), place(shape, target[one])) for one in devices]


def step_moves(shape, turn, east):
    nx, ny, _ = shape
    moves = {}
    for a in range(nx):
        for b in range(ny):
            if (a + b) % PERIOD == turn % PERIOD:
                if east and a + 1 < nx:
                    moves[a, b, 0] = (a + 1, b, 0)
                if not east and b + 1 < ny:
                    moves[a, b, 0] = (a, b + 1, 0)
                if east and a == 0 and b % 2 == 0:
                    moves[a, b + 1, 1] = (a, b + 1, 0)
    return completed(shape, moves)


def step_body(turn, west_ref, south_ref, own_ref, other_ref, forward_ref, west_in, south_in, east_ref, north_ref, west_all, south_all):
    modes = west_ref.shape[1]
    a, b, row = (lax.axis_index(axis) for axis in AXES)

    @pl.when(jnp.logical_and(a + b == turn, row == 0))
    def _():
        west = jnp.where(a > 0, west_ref[...], jnp.zeros_like(west_ref))
        south = jnp.where(b > 0, south_ref[...], jnp.zeros_like(south_ref))
        west_all[...] = west
        south_all[...] = south
        source = jnp.concatenate([own_ref[...], other_ref[...]], 0)
        left = (source[:, :modes].astype(jnp.float32) + west.astype(jnp.float32)).astype(jnp.bfloat16)
        right = (source[:, modes:].astype(jnp.float32) + south.astype(jnp.float32)).astype(jnp.bfloat16)
        inflow = jnp.concatenate([left, right], 1)
        east_ref[...] = jnp.dot(inflow, forward_ref[:, :modes], preferred_element_type=jnp.float32).astype(jnp.bfloat16)
        north_ref[...] = jnp.dot(inflow, forward_ref[:, modes:], preferred_element_type=jnp.float32).astype(jnp.bfloat16)


def step(turn, west, south, own, other, forward, west_all, south_all):
    rows, modes = west.shape
    vmem = pl.BlockSpec(memory_space=pltpu.VMEM)
    arrays = [pltpu.with_memory_space_constraint(i, pltpu.VMEM) for i in (west, south, own, other, forward, west_all, south_all)]
    return pl.pallas_call(
        functools.partial(step_body, turn),
        out_shape=[pltpu.VMEM((rows, modes), jnp.bfloat16)] * 4,
        in_specs=[vmem] * 7,
        out_specs=[vmem] * 4,
        input_output_aliases={5: 2, 6: 3},
        cost_estimate=pl.CostEstimate(flops=8 * rows * modes * modes, bytes_accessed=8 * modes * modes, transcendentals=0),
        compiler_params=pltpu.CompilerParams(vmem_limit_bytes=4 * 1024 * 1024),
    )(*arrays)


def on_device(shape, sources, scatter):
    nx, ny, nr = shape
    own = sources[0, 0]
    columns = scatter[0, 0]
    rows, width = own.shape
    modes = width // 2
    cells = [(i, j, k) for i in range(nx) for j in range(ny) for k in range(nr)]
    across = [(place(shape, (i, j, k)), place(shape, (i, j, 1 - k))) for i, j, k in cells]
    other = lax.ppermute(own, AXES, across)
    face = jnp.zeros((2 * rows, modes), jnp.bfloat16)
    west, south, west_all, south_all = face, face, face, face
    turns = nx + ny - 1
    for t in range(turns):
        east, north, west_all, south_all = step(t, west, south, own, other, columns, west_all, south_all)
        if t < turns - 1:
            west = lax.ppermute(east, AXES, step_moves(shape, t, True))
            south = lax.ppermute(north, AXES, step_moves(shape, t, False))
    row = lax.axis_index("row")
    faces = jnp.concatenate([west_all, south_all], 1)
    sent = lax.ppermute(faces, AXES, across)
    faces = jnp.where(row == 0, faces, sent)
    source = jnp.where(row == 0, jnp.concatenate([own, other], 0), jnp.concatenate([other, own], 0))
    inflow = source.astype(jnp.float32) + faces.astype(jnp.float32)
    back = jnp.dot(inflow.astype(jnp.bfloat16), columns, preferred_element_type=jnp.float32).astype(jnp.bfloat16)

    def returned(value, da, db, flip):
        pairs = [(place(shape, (i, j, k)), place(shape, ((i - da) % nx, (j - db) % ny, k ^ flip))) for i, j, k in cells]
        return lax.ppermute(value, AXES, pairs)

    from_east = jnp.where(
        row == 0, returned(back[:rows, :modes], 1, 0, 1), returned(back[rows:, :modes], 1, 0, 0)
    )
    from_north = jnp.where(
        row == 0, returned(back[:rows, modes:], 0, 1, 1), returned(back[rows:, modes:], 0, 1, 0)
    )
    from_east = jnp.where(lax.axis_index("gx") < nx - 1, from_east, 0)
    from_north = jnp.where(lax.axis_index("gy") < ny - 1, from_north, 0)
    mine = jnp.where(row == 0, inflow[:rows], inflow[rows:])
    traces = mine + jnp.concatenate([from_east, from_north], 1).astype(jnp.float32)
    return traces[None, None]


def solution(mesh):
    shape = tuple(mesh.shape[axis] for axis in AXES)
    placed = (P("gx", "gy", "row", None), P("gx", "gy", None, "row"))
    return jax.shard_map(
        functools.partial(on_device, shape), mesh=mesh, in_specs=placed, out_specs=P("gx", "gy", "row", None), check_vma=False
    )
```

```python
import functools

import jax
import jax.numpy as jnp
from jax import lax
from jax.experimental import pallas as pl
from jax.experimental.pallas import tpu as pltpu
from jax.sharding import PartitionSpec as P


AXES = ("gx", "gy", "row")
PERIOD = 15


def place(shape, cell):
    a, b, row = cell
    return (a * shape[1] + b) * shape[2] + row


def step_moves(shape, turn, east):
    nx, ny, _ = shape
    turn %= PERIOD
    target = {}

    def cycle(*devices):
        for one, two in zip(devices, devices[1:] + devices[:1]):
            target[one] = two

    now = [(a, b) for a in range(nx) for b in range(ny) if (a + b - turn) % PERIOD == 0]
    after = [(a, b) for a in range(nx) for b in range(ny) if (a + b - turn) % PERIOD == 1]
    busy = {(a, b // 2) for a, b in now + after}

    def away(real):
        if real:
            options = [(c, (turn // 2 + k) % 4) for k in range(4) for c in (turn % 2, 1 - turn % 2, 2)]
        else:
            options = [((0, 6), (2, 5), (1, 6), (3, 5), (4, 4), (0, 6), (2, 5))[turn]] if turn < 7 else []
        for c, k in options:
            if (c, k) not in busy:
                busy.add((c, k))
                return (c, 2 * k, 1), (c, 2 * k + 1, 1)
        return None

    for a, b in after:
        came = (a - 1, b) if east else (a, b - 1)
        if b % 2 == 0:
            if min(came) >= 0:
                cycle(came + (0,), (a, b, 0), (a, b + 1, 0), (a, b + 1, 1), (a, b, 1))
            else:
                cycle((a, b, 0), (a, b + 1, 0))
                cycle((a, b + 1, 1), (a, b, 1))
        elif not east:
            cycle(came + (0,), (a, b, 0))
        elif min(came) >= 0:
            cycle(came + (0,), (a, b, 0), (a, b, 1))
        elif b + 1 < ny and (a, b // 2 + 1) not in busy:
            busy.add((a, b // 2 + 1))
            cycle((a, b, 0), (a, b + 1, 0), (a, b + 2, 0))
            cycle((a, b + 1, 1), (a, b + 2, 1))
        else:
            cycle((a, b, 0), (a, b, 1))
    for a, b in now:
        if (a, b, 0) not in target:
            chip = away(a + b == turn) if east else None
            if chip:
                cycle((a, b, 0), *chip)
    cells = [(a, b, row) for a in range(nx) for row in range(2) for b in range(ny)]
    for a, b, row in cells:
        if (a, b, row) not in target and b % 2 == 0 and (a, b + 1, row) not in target:
            if (a, b // 2) not in busy or row == 0:
                cycle((a, b, row), (a, b + 1, row))
    for real in (True, False):
        left = [i for i in cells if i not in target and (abs(i[0] + i[1] - turn) < 4) == real]
        if len(left) == 1:
            a, b = next(i for i in (sorted if real else reversed)(sorted({c[:2] for c in cells})) if target.get(i + (1,)) == (i[0], i[1] ^ 1, 1) and i[1] % 2 == 0 and (i[0], i[1] // 2) not in busy)
            left += [(a, b, 1), (a, b + 1, 1)]
        groups = []
        for a in range(nx):
            column = [i for i in left if i[0] == a]
            if groups and (len(groups[-1]) == 1 or len(column) == 1):
                groups[-1] += column
            elif column:
                groups.append(column)
        for group in groups:
            cycle(*group)
    return [(place(shape, one), place(shape, target[one])) for one in sorted(target)]


def load_body(scatter_ref, own_ref, columns_ref, rows_ref, sem):
    first = pltpu.make_async_copy(scatter_ref, columns_ref, sem.at[0])
    second = pltpu.make_async_copy(own_ref, rows_ref, sem.at[1])
    first.start()
    second.start()
    first.wait()
    second.wait()


def load(columns, own):
    vmem = pl.BlockSpec(memory_space=pltpu.VMEM)
    return pl.pallas_call(
        load_body,
        out_shape=[pltpu.VMEM(columns.shape, columns.dtype), pltpu.VMEM(own.shape, own.dtype)],
        in_specs=[pl.BlockSpec(memory_space=pltpu.HBM)] * 2,
        out_specs=[vmem] * 2,
        scratch_shapes=[pltpu.SemaphoreType.DMA((2,))],
        cost_estimate=pl.CostEstimate(flops=3 * 10**9, bytes_accessed=4 * columns.size, transcendentals=0),
        compiler_params=pltpu.CompilerParams(vmem_limit_bytes=1024 * 1024),
    )(pltpu.with_memory_space_constraint(columns, pltpu.HBM), pltpu.with_memory_space_constraint(own, pltpu.HBM))


def combine_body(own_ref, west_ref, south_ref, source_ref):
    rows, modes = west_ref.shape
    mine = lax.axis_index(AXES[2]) * rows
    theirs = rows - mine
    source_ref[pl.ds(pl.multiple_of(mine, rows), rows), :] = own_ref[...]
    source_ref[pl.ds(pl.multiple_of(theirs, rows), rows), :modes] = west_ref[...]
    source_ref[pl.ds(pl.multiple_of(theirs, rows), rows), modes:] = south_ref[...]


def combine(own, west, south):
    vmem = pl.BlockSpec(memory_space=pltpu.VMEM)
    arrays = [pltpu.with_memory_space_constraint(i, pltpu.VMEM) for i in (own, west, south)]
    return pl.pallas_call(
        combine_body,
        out_shape=pltpu.VMEM((2 * own.shape[0], own.shape[1]), own.dtype),
        in_specs=[vmem] * 3,
        out_specs=vmem,
        compiler_params=pltpu.CompilerParams(vmem_limit_bytes=1024 * 1024),
    )(*arrays)


def step_body(turn_in, west_ref, south_ref, source_ref, forward_ref, west_in, south_in, sent_ref, west_all, south_all, turn_ref, inflow):
    rows, modes = west_ref.shape
    a, b, row = (lax.axis_index(axis) for axis in AXES)

    turn = turn_in[0]
    turn_ref[0] = turn + 1

    @pl.when(jnp.logical_and(a + b == turn, row == 0))
    def _():
        @pl.loop(0, rows // 16)
        def _(i):
            part = pl.ds(pl.multiple_of(i * 16, 16), 16)
            west = jnp.where(a > 0, west_ref[part], 0)
            south = jnp.where(b > 0, south_ref[part], 0)
            west_all[part] = west
            south_all[part] = south
            inflow[part, :modes] = (source_ref[part, :modes].astype(jnp.float32) + west.astype(jnp.float32)).astype(jnp.bfloat16)
            inflow[part, modes:] = (source_ref[part, modes:].astype(jnp.float32) + south.astype(jnp.float32)).astype(jnp.bfloat16)

        @pl.loop(0, 2)
        def _(i):
            columns = pl.ds(pl.multiple_of(i * modes, modes), modes)
            sent_ref[:, columns] = jnp.dot(inflow[...], forward_ref[:, columns], preferred_element_type=jnp.float32).astype(jnp.bfloat16)


def step(turn, west, south, source, forward, west_all, south_all):
    rows, modes = west.shape
    vmem = pl.BlockSpec(memory_space=pltpu.VMEM)
    arrays = [pltpu.with_memory_space_constraint(i, pltpu.VMEM) for i in (west, south, source, forward, west_all, south_all)]
    face = pltpu.VMEM((rows, modes), jnp.bfloat16)
    smem = pl.BlockSpec(memory_space=pltpu.SMEM)
    sent, west_all, south_all, turn = pl.pallas_call(
        step_body,
        out_shape=[pltpu.VMEM((rows, 2 * modes), jnp.bfloat16), face, face, pltpu.SMEM((1,), jnp.int32)],
        in_specs=[smem] + [vmem] * 6,
        out_specs=[vmem] * 3 + [smem],
        scratch_shapes=[pltpu.VMEM((rows, 2 * modes), jnp.bfloat16)],
        input_output_aliases={5: 1, 6: 2},
        cost_estimate=pl.CostEstimate(flops=8 * rows * modes * modes, bytes_accessed=8 * modes * modes, transcendentals=0),
        compiler_params=pltpu.CompilerParams(vmem_limit_bytes=4 * 1024 * 1024),
    )(pltpu.with_memory_space_constraint(turn, pltpu.SMEM), *arrays)
    return sent[:, :modes], sent[:, modes:], west_all, south_all, turn


def keep_body(turn, west_ref, south_ref, west_in, south_in, west_all, south_all):
    a, b, row = (lax.axis_index(axis) for axis in AXES)

    @pl.when(jnp.logical_and(a + b == turn, row == 0))
    def _():
        west_all[...] = west_ref[...]
        south_all[...] = south_ref[...]


def keep(turn, west, south, west_all, south_all):
    vmem = pl.BlockSpec(memory_space=pltpu.VMEM)
    face = pltpu.VMEM(west.shape, west.dtype)
    arrays = [pltpu.with_memory_space_constraint(i, pltpu.VMEM) for i in (west, south, west_all, south_all)]
    return pl.pallas_call(
        functools.partial(keep_body, turn),
        out_shape=[face] * 2,
        in_specs=[vmem] * 4,
        out_specs=[vmem] * 2,
        input_output_aliases={2: 0, 3: 1},
        compiler_params=pltpu.CompilerParams(vmem_limit_bytes=1024 * 1024),
    )(*arrays)


def reflect_body(west_own, south_own, west_got, south_got, source_ref, columns_ref, mine_ref, west_low, west_high, south_low, south_high, inflow):
    rows, modes = west_own.shape
    half = rows // 2
    row = lax.axis_index(AXES[2])
    faces = ((west_own, west_got, slice(0, modes)), (south_own, south_got, slice(modes, 2 * modes)))

    @pl.when(row == 0)
    def _():
        for own, _, part in faces:
            mine_ref[:, part] = source_ref[:half, part].astype(jnp.float32) + own[:half].astype(jnp.float32)

    @pl.when(row == 1)
    def _():
        for _, got, part in faces:
            value = source_ref[:, part].astype(jnp.float32) + got[...].astype(jnp.float32)
            mine_ref[:, part] = value[half:]
            inflow[:, part] = value.astype(jnp.bfloat16)
        for low, high, part in ((west_low, west_high, faces[0][2]), (south_low, south_high, faces[1][2])):
            back = jnp.dot(inflow[...], columns_ref[:, part], preferred_element_type=jnp.float32).astype(jnp.bfloat16)
            low[...] = back[:half]
            high[...] = back[half:]


def reflect(*arrays):
    rows, modes = arrays[0].shape
    vmem = pl.BlockSpec(memory_space=pltpu.VMEM)
    return pl.pallas_call(
        reflect_body,
        out_shape=[pltpu.VMEM((rows // 2, 2 * modes), jnp.float32)] + [pltpu.VMEM((rows // 2, modes), jnp.bfloat16)] * 4,
        in_specs=[vmem] * 6,
        out_specs=[vmem] * 5,
        scratch_shapes=[pltpu.VMEM((rows, 2 * modes), jnp.bfloat16)],
        cost_estimate=pl.CostEstimate(flops=8 * rows * modes * modes, bytes_accessed=8 * modes * modes, transcendentals=0),
        compiler_params=pltpu.CompilerParams(vmem_limit_bytes=4 * 1024 * 1024),
    )(*[pltpu.with_memory_space_constraint(i, pltpu.VMEM) for i in arrays])


def total_body(shape, mine_ref, west_low, west_high, south_low, south_high, out_ref):
    modes = west_low.shape[1]
    a, b, row = (lax.axis_index(axis) for axis in AXES)
    sides = ((west_low, west_high, slice(0, modes), a < shape[0] - 1), (south_low, south_high, slice(modes, 2 * modes), b < shape[1] - 1))
    for low, high, part, inside in sides:
        for k, ref in enumerate((low, high)):

            @pl.when(jnp.logical_and(row == k, inside))
            def _():
                out_ref[:, part] = mine_ref[:, part] + ref[...].astype(jnp.float32)

        @pl.when(jnp.logical_not(inside))
        def _():
            out_ref[:, part] = mine_ref[:, part]


def total(shape, *arrays):
    vmem = pl.BlockSpec(memory_space=pltpu.VMEM)
    return pl.pallas_call(
        functools.partial(total_body, shape),
        out_shape=jax.ShapeDtypeStruct(arrays[0].shape, jnp.float32),
        in_specs=[vmem] * 5,
        out_specs=vmem,
        compiler_params=pltpu.CompilerParams(vmem_limit_bytes=4 * 1024 * 1024),
    )(*[pltpu.with_memory_space_constraint(i, pltpu.VMEM) for i in arrays])


def back_moves(shape, west, high):
    nx, ny, _ = shape
    count = nx if west else ny
    target = {}
    for a in range(nx):
        for b in range(ny):
            k = a if west else b

            def at(step, row):
                return (a + step, b, row) if west else (a, b + step, row)

            if high:
                target[a, b, 1] = at(-1, 1) if k > 0 else at(0, 0)
                target[a, b, 0] = at(1, 0) if k < count - 1 else at(0, 1)
            else:
                mate = (a, b ^ 1) if west else (a ^ 1, b)
                target[a, b, 1] = at(-1, 0) if k > 0 else mate + (1,)
                target[a, b, 0] = at(1, 1) if k < count - 1 else mate + (0,)
    return [(place(shape, one), place(shape, target[one])) for one in sorted(target)]


def on_device(shape, sources, scatter):
    nx, ny, nr = shape
    own = sources[0, 0]
    columns = scatter[0, 0]
    rows, width = own.shape
    modes = width // 2
    cells = [(i, j, k) for i in range(nx) for j in range(ny) for k in range(nr)]
    across = [(place(shape, (i, j, k)), place(shape, (i, j, 1 - k))) for i, j, k in cells]
    other = [lax.ppermute(own[:, half : half + modes], AXES, across) for half in (0, modes)]
    columns, own = load(columns, own)
    source = combine(own, *other)
    face = jnp.zeros((2 * rows, modes), jnp.bfloat16)
    east, north, west_all, south_all, turn = step(jnp.zeros((1,), jnp.int32), face, face, source, columns, face, face)
    for t in range(nx + ny - 2):
        west = lax.ppermute(east, AXES, step_moves(shape, t, True))
        south = lax.ppermute(north, AXES, step_moves(shape, t, False))
        if t < nx + ny - 3:
            east, north, west_all, south_all, turn = step(turn, west, south, source, columns, west_all, south_all)
    west_all, south_all = keep(nx + ny - 2, west, south, west_all, south_all)
    west_got, south_got = (lax.ppermute(face, AXES, across) for face in (west_all, south_all))
    mine, *parts = reflect(west_all, south_all, west_got, south_got, source, columns)
    order = ((0, True, False), (2, False, False), (1, True, True), (3, False, True))
    returned = {k: lax.ppermute(parts[k], AXES, back_moves(shape, west, high)) for k, west, high in order}
    return total(shape, mine, *[returned[k] for k in range(4)])[None, None]


def solution(mesh):
    shape = tuple(mesh.shape[axis] for axis in AXES)
    placed = (P("gx", "gy", "row", None), P("gx", "gy", None, "row"))
    return jax.shard_map(
        functools.partial(on_device, shape), mesh=mesh, in_specs=placed, out_specs=P("gx", "gy", "row", None), check_vma=False
    )
```

```python
import functools

import jax
import jax.numpy as jnp
from jax import lax
from jax.experimental import pallas as pl
from jax.experimental.pallas import tpu as pltpu
from jax.sharding import PartitionSpec as P


AXES = ("gx", "gy", "row")
PERIOD = 15


def place(shape, cell):
    a, b, row = cell
    return (a * shape[1] + b) * shape[2] + row


def step_moves(shape, turn, east):
    nx, ny, _ = shape
    turn %= PERIOD
    target = {}

    def cycle(*devices):
        for one, two in zip(devices, devices[1:] + devices[:1]):
            target[one] = two

    now = [(a, b) for a in range(nx) for b in range(ny) if (a + b - turn) % PERIOD == 0]
    after = [(a, b) for a in range(nx) for b in range(ny) if (a + b - turn) % PERIOD == 1]
    busy = {(a, b // 2) for a, b in now + after}

    def away(real):
        if real:
            options = [(c, (turn // 2 + k) % 4) for k in range(4) for c in (turn % 2, 1 - turn % 2, 2)]
        else:
            options = [((0, 6), (2, 5), (1, 6), (3, 5), (4, 4), (5, 4), (2, 5))[turn]] if turn < 7 else []
        for c, k in options:
            if (c, k) not in busy:
                busy.add((c, k))
                return (c, 2 * k, 1), (c, 2 * k + 1, 1)
        return None

    for a, b in after:
        came = (a - 1, b) if east else (a, b - 1)
        if a + b == nx + ny - 2:
            cycle(came + (0,), (a, b, 0))
            if east:
                cycle((a - 1, b - 1, 0), (a, b - 1, 0))
                cycle((a - 1, b - 1, 1), (a - 1, b, 1))
                cycle((a, b - 1, 1), (a, b, 1))
            continue
        if b % 2 == 0:
            if min(came) >= 0:
                cycle(came + (0,), (a, b, 0), (a, b + 1, 0), (a, b + 1, 1), (a, b, 1))
            else:
                cycle((a, b, 0), (a, b + 1, 0))
                cycle((a, b + 1, 1), (a, b, 1))
        elif not east:
            cycle(came + (0,), (a, b, 0))
        elif min(came) >= 0:
            cycle(came + (0,), (a, b, 0), (a, b, 1))
        elif b + 1 < ny and (a, b // 2 + 1) not in busy:
            busy.add((a, b // 2 + 1))
            cycle((a, b, 0), (a, b + 1, 0), (a, b + 2, 0))
            cycle((a, b + 1, 1), (a, b + 2, 1))
        else:
            cycle((a, b, 0), (a, b, 1))
    for a, b in now:
        if (a, b, 0) not in target:
            chip = away(a + b == turn) if east else None
            if chip:
                cycle((a, b, 0), *chip)
    cells = [(a, b, row) for a in range(nx) for row in range(2) for b in range(ny)]
    for a, b, row in cells:
        if (a, b, row) not in target and b % 2 == 0 and (a, b + 1, row) not in target:
            if (a, b // 2) not in busy or row == 0:
                cycle((a, b, row), (a, b + 1, row))
    for real in (True, False):
        left = [i for i in cells if i not in target and (abs(i[0] + i[1] - turn) < 4) == real]
        if len(left) == 1:
            a, b = next(i for i in (sorted if real else reversed)(sorted({c[:2] for c in cells})) if target.get(i + (1,)) == (i[0], i[1] ^ 1, 1) and i[1] % 2 == 0 and (i[0], i[1] // 2) not in busy)
            left += [(a, b, 1), (a, b + 1, 1)]
        groups = []
        for a in range(nx):
            column = [i for i in left if i[0] == a]
            if groups and (len(groups[-1]) == 1 or len(column) == 1):
                groups[-1] += column
            elif column:
                groups.append(column)
        for group in groups:
            cycle(*group)
    return [(place(shape, one), place(shape, target[one])) for one in sorted(target)]


def load_body(scatter_ref, own_ref, columns_ref, rows_ref, sem):
    first = pltpu.make_async_copy(scatter_ref, columns_ref, sem.at[0])
    second = pltpu.make_async_copy(own_ref, rows_ref, sem.at[1])
    first.start()
    second.start()
    first.wait()
    second.wait()


def load(columns, own):
    vmem = pl.BlockSpec(memory_space=pltpu.VMEM)
    return pl.pallas_call(
        load_body,
        out_shape=[pltpu.VMEM(columns.shape, columns.dtype), pltpu.VMEM(own.shape, own.dtype)],
        in_specs=[pl.BlockSpec(memory_space=pltpu.HBM)] * 2,
        out_specs=[vmem] * 2,
        scratch_shapes=[pltpu.SemaphoreType.DMA((2,))],
        cost_estimate=pl.CostEstimate(flops=3 * 10**9, bytes_accessed=4 * columns.size, transcendentals=0),
        compiler_params=pltpu.CompilerParams(vmem_limit_bytes=1024 * 1024),
    )(pltpu.with_memory_space_constraint(columns, pltpu.HBM), pltpu.with_memory_space_constraint(own, pltpu.HBM))


def combine_body(own_ref, other_ref, source_ref):
    rows = own_ref.shape[0]
    mine = lax.axis_index(AXES[2]) * rows
    source_ref[pl.ds(pl.multiple_of(mine, rows), rows), :] = own_ref[...]
    source_ref[pl.ds(pl.multiple_of(rows - mine, rows), rows), :] = other_ref[...]


def combine(own, other):
    vmem = pl.BlockSpec(memory_space=pltpu.VMEM)
    arrays = [pltpu.with_memory_space_constraint(i, pltpu.VMEM) for i in (own, other)]
    return pl.pallas_call(
        combine_body,
        out_shape=pltpu.VMEM((2 * own.shape[0], own.shape[1]), own.dtype),
        in_specs=[vmem] * 2,
        out_specs=vmem,
        compiler_params=pltpu.CompilerParams(vmem_limit_bytes=1024 * 1024),
    )(*arrays)


def step_body(turn_in, west_ref, south_ref, source_ref, forward_ref, west_in, south_in, sent_ref, west_all, south_all, turn_ref, inflow):
    rows, modes = west_ref.shape
    a, b, row = (lax.axis_index(axis) for axis in AXES)

    turn = turn_in[0]
    turn_ref[0] = turn + 1

    @pl.when(jnp.logical_and(a + b == turn, row == 0))
    def _():
        @pl.loop(0, rows // 16)
        def _(i):
            part = pl.ds(pl.multiple_of(i * 16, 16), 16)
            west = jnp.where(a > 0, west_ref[part], 0)
            south = jnp.where(b > 0, south_ref[part], 0)
            west_all[part] = west
            south_all[part] = south
            inflow[part, :modes] = (source_ref[part, :modes].astype(jnp.float32) + west.astype(jnp.float32)).astype(jnp.bfloat16)
            inflow[part, modes:] = (source_ref[part, modes:].astype(jnp.float32) + south.astype(jnp.float32)).astype(jnp.bfloat16)

        @pl.loop(0, 2)
        def _(i):
            columns = pl.ds(pl.multiple_of(i * modes, modes), modes)
            sent_ref[:, columns] = jnp.dot(inflow[...], forward_ref[:, columns], preferred_element_type=jnp.float32).astype(jnp.bfloat16)


def step(turn, west, south, source, forward, west_all, south_all):
    rows, modes = west.shape
    vmem = pl.BlockSpec(memory_space=pltpu.VMEM)
    arrays = [pltpu.with_memory_space_constraint(i, pltpu.VMEM) for i in (west, south, source, forward, west_all, south_all)]
    face = pltpu.VMEM((rows, modes), jnp.bfloat16)
    smem = pl.BlockSpec(memory_space=pltpu.SMEM)
    sent, west_all, south_all, turn = pl.pallas_call(
        step_body,
        out_shape=[pltpu.VMEM((rows, 2 * modes), jnp.bfloat16), face, face, pltpu.SMEM((1,), jnp.int32)],
        in_specs=[smem] + [vmem] * 6,
        out_specs=[vmem] * 3 + [smem],
        scratch_shapes=[pltpu.VMEM((rows, 2 * modes), jnp.bfloat16)],
        input_output_aliases={5: 1, 6: 2},
        cost_estimate=pl.CostEstimate(flops=8 * rows * modes * modes, bytes_accessed=8 * modes * modes, transcendentals=0),
        compiler_params=pltpu.CompilerParams(vmem_limit_bytes=4 * 1024 * 1024),
    )(pltpu.with_memory_space_constraint(turn, pltpu.SMEM), *arrays)
    return sent[:, :modes], sent[:, modes:], west_all, south_all, turn


def keep_body(turn, west_ref, south_ref, west_all, south_all, faces_ref):
    modes = west_ref.shape[1]
    a, b, row = (lax.axis_index(axis) for axis in AXES)
    last = jnp.logical_and(a + b == turn, row == 0)
    for now, kept, part in ((west_ref, west_all, slice(0, modes)), (south_ref, south_all, slice(modes, 2 * modes))):

        @pl.when(last)
        def _():
            faces_ref[:, part] = now[...]

        @pl.when(jnp.logical_not(last))
        def _():
            faces_ref[:, part] = kept[...]


def keep(turn, west, south, west_all, south_all):
    vmem = pl.BlockSpec(memory_space=pltpu.VMEM)
    arrays = [pltpu.with_memory_space_constraint(i, pltpu.VMEM) for i in (west, south, west_all, south_all)]
    return pl.pallas_call(
        functools.partial(keep_body, turn),
        out_shape=pltpu.VMEM((west.shape[0], 2 * west.shape[1]), west.dtype),
        in_specs=[vmem] * 4,
        out_specs=vmem,
        compiler_params=pltpu.CompilerParams(vmem_limit_bytes=1024 * 1024),
    )(*arrays)


def reflect_body(faces_own, faces_got, source_ref, columns_ref, mine_ref, west_low, west_high, south_low, south_high, inflow):
    rows, width = faces_own.shape
    half, modes = rows // 2, width // 2
    row = lax.axis_index(AXES[2])

    @pl.when(row == 0)
    def _():
        mine_ref[...] = source_ref[:half].astype(jnp.float32) + faces_own[:half].astype(jnp.float32)

    @pl.when(row == 1)
    def _():
        @pl.loop(0, rows // 16)
        def _(i):
            part = pl.ds(pl.multiple_of(i * 16, 16), 16)
            inflow[part] = (source_ref[part].astype(jnp.float32) + faces_got[part].astype(jnp.float32)).astype(jnp.bfloat16)

        for k, (low, high) in enumerate(((west_low, west_high), (south_low, south_high))):
            back = jnp.dot(inflow[...], columns_ref[:, k * modes : (k + 1) * modes], preferred_element_type=jnp.float32).astype(jnp.bfloat16)
            low[...] = back[:half]
            high[...] = back[half:]
        mine_ref[...] = source_ref[half:].astype(jnp.float32) + faces_got[half:].astype(jnp.float32)


def reflect(*arrays):
    rows, modes = arrays[0].shape[0], arrays[0].shape[1] // 2
    vmem = pl.BlockSpec(memory_space=pltpu.VMEM)
    return pl.pallas_call(
        reflect_body,
        out_shape=[pltpu.VMEM((rows // 2, 2 * modes), jnp.float32)] + [pltpu.VMEM((rows // 2, modes), jnp.bfloat16)] * 4,
        in_specs=[vmem] * 4,
        out_specs=[vmem] * 5,
        scratch_shapes=[pltpu.VMEM((rows, 2 * modes), jnp.bfloat16)],
        cost_estimate=pl.CostEstimate(flops=8 * rows * modes * modes, bytes_accessed=8 * modes * modes, transcendentals=0),
        compiler_params=pltpu.CompilerParams(vmem_limit_bytes=4 * 1024 * 1024),
    )(*[pltpu.with_memory_space_constraint(i, pltpu.VMEM) for i in arrays])


def total_body(shape, mine_ref, west_low, west_high, south_low, south_high, out_ref):
    modes = west_low.shape[1]
    a, b, row = (lax.axis_index(axis) for axis in AXES)
    sides = ((west_low, west_high, slice(0, modes), a < shape[0] - 1), (south_low, south_high, slice(modes, 2 * modes), b < shape[1] - 1))
    for low, high, part, inside in sides:
        for k, ref in enumerate((low, high)):

            @pl.when(jnp.logical_and(row == k, inside))
            def _():
                out_ref[:, part] = mine_ref[:, part] + ref[...].astype(jnp.float32)

        @pl.when(jnp.logical_not(inside))
        def _():
            out_ref[:, part] = mine_ref[:, part]


def total(shape, *arrays):
    vmem = pl.BlockSpec(memory_space=pltpu.VMEM)
    return pl.pallas_call(
        functools.partial(total_body, shape),
        out_shape=jax.ShapeDtypeStruct(arrays[0].shape, jnp.float32),
        in_specs=[vmem] * 5,
        out_specs=vmem,
        compiler_params=pltpu.CompilerParams(vmem_limit_bytes=4 * 1024 * 1024),
    )(*[pltpu.with_memory_space_constraint(i, pltpu.VMEM) for i in arrays])


def back_moves(shape, west, high):
    nx, ny, _ = shape
    count = nx if west else ny
    target = {}
    for a in range(nx):
        for b in range(ny):
            k = a if west else b

            def at(step, row):
                return (a + step, b, row) if west else (a, b + step, row)

            if high:
                target[a, b, 1] = at(-1, 1) if k > 0 else at(0, 0)
                target[a, b, 0] = at(1, 0) if k < count - 1 else at(0, 1)
            else:
                mate = (a, b ^ 1) if west else (a ^ 1, b)
                target[a, b, 1] = at(-1, 0) if k > 0 else mate + (1,)
                target[a, b, 0] = at(1, 1) if k < count - 1 else mate + (0,)
    return [(place(shape, one), place(shape, target[one])) for one in sorted(target)]


def on_device(shape, sources, scatter):
    nx, ny, nr = shape
    own = sources[0, 0]
    columns = scatter[0, 0]
    rows, width = own.shape
    modes = width // 2
    cells = [(i, j, k) for i in range(nx) for j in range(ny) for k in range(nr)]
    across = [(place(shape, (i, j, k)), place(shape, (i, j, 1 - k))) for i, j, k in cells]
    other = lax.ppermute(own, AXES, across)
    columns, own = load(columns, own)
    source = combine(own, other)
    face = jnp.zeros((2 * rows, modes), jnp.bfloat16)
    east, north, west_all, south_all, turn = step(jnp.zeros((1,), jnp.int32), face, face, source, columns, face, face)
    for t in range(nx + ny - 2):
        west = lax.ppermute(east, AXES, step_moves(shape, t, True))
        south = lax.ppermute(north, AXES, step_moves(shape, t, False))
        if t < nx + ny - 3:
            east, north, west_all, south_all, turn = step(turn, west, south, source, columns, west_all, south_all)
    faces = keep(nx + ny - 2, west, south, west_all, south_all)
    mine, *parts = reflect(faces, lax.ppermute(faces, AXES, across[::2]), source, columns)
    returned = {}
    for k, west, high in ((0, True, False), (2, False, False), (1, True, True), (3, False, True)):
        returned[k] = lax.ppermute(parts[k], AXES, back_moves(shape, west, high))
    return total(shape, mine, *[returned[k] for k in range(4)])[None, None]


def solution(mesh):
    shape = tuple(mesh.shape[axis] for axis in AXES)
    placed = (P("gx", "gy", "row", None), P("gx", "gy", None, "row"))
    return jax.shard_map(
        functools.partial(on_device, shape), mesh=mesh, in_specs=placed, out_specs=P("gx", "gy", "row", None), check_vma=False
    )
```

```python
import functools

import jax
import jax.numpy as jnp
from jax import lax
from jax.experimental import pallas as pl
from jax.experimental.pallas import tpu as pltpu
from jax.sharding import PartitionSpec as P


AXES = ("gx", "gy", "row")
PERIOD = 15


def place(shape, cell):
    a, b, row = cell
    return (a * shape[1] + b) * shape[2] + row


def step_moves(shape, turn, east):
    nx, ny, _ = shape
    turn %= PERIOD
    target = {}

    def cycle(*devices):
        for one, two in zip(devices, devices[1:] + devices[:1]):
            target[one] = two

    now = [(a, b) for a in range(nx) for b in range(ny) if (a + b - turn) % PERIOD == 0]
    after = [(a, b) for a in range(nx) for b in range(ny) if (a + b - turn) % PERIOD == 1]
    busy = {(a, b // 2) for a, b in now + after}

    def away(real):
        if real:
            options = [(c, (turn // 2 + k) % 4) for k in range(4) for c in (turn % 2, 1 - turn % 2, 2)]
        else:
            options = [((0, 6), (2, 5), (1, 6), (3, 5), (4, 4), (5, 4), (2, 5))[turn]] if turn < 7 else []
        for c, k in options:
            if (c, k) not in busy:
                busy.add((c, k))
                return (c, 2 * k, 1), (c, 2 * k + 1, 1)
        return None

    for a, b in after:
        came = (a - 1, b) if east else (a, b - 1)
        if a + b == nx + ny - 2:
            cycle(came + (0,), (a, b, 0))
            if east:
                cycle((a - 1, b - 1, 0), (a, b - 1, 0))
                cycle((a - 1, b - 1, 1), (a - 1, b, 1))
                cycle((a, b - 1, 1), (a, b, 1))
            continue
        if b % 2 == 0:
            if min(came) >= 0:
                cycle(came + (0,), (a, b, 0), (a, b + 1, 0), (a, b + 1, 1), (a, b, 1))
            else:
                cycle((a, b, 0), (a, b + 1, 0))
                cycle((a, b + 1, 1), (a, b, 1))
        elif not east:
            cycle(came + (0,), (a, b, 0))
        elif min(came) >= 0:
            cycle(came + (0,), (a, b, 0), (a, b, 1))
        elif b + 1 < ny and (a, b // 2 + 1) not in busy:
            busy.add((a, b // 2 + 1))
            cycle((a, b, 0), (a, b + 1, 0), (a, b + 2, 0))
            cycle((a, b + 1, 1), (a, b + 2, 1))
        else:
            cycle((a, b, 0), (a, b, 1))
    for a, b in now:
        if (a, b, 0) not in target:
            chip = away(a + b == turn) if east else None
            if chip:
                cycle((a, b, 0), *chip)
    cells = [(a, b, row) for a in range(nx) for row in range(2) for b in range(ny)]
    for a, b, row in cells:
        if (a, b, row) not in target and b % 2 == 0 and (a, b + 1, row) not in target:
            if (a, b // 2) not in busy or row == 0:
                cycle((a, b, row), (a, b + 1, row))
    for real in (True, False):
        left = [i for i in cells if i not in target and (abs(i[0] + i[1] - turn) < 4) == real]
        if len(left) == 1:
            a, b = next(i for i in (sorted if real else reversed)(sorted({c[:2] for c in cells})) if target.get(i + (1,)) == (i[0], i[1] ^ 1, 1) and i[1] % 2 == 0 and (i[0], i[1] // 2) not in busy)
            left += [(a, b, 1), (a, b + 1, 1)]
        groups = []
        for a in range(nx):
            column = [i for i in left if i[0] == a]
            if groups and (len(groups[-1]) == 1 or len(column) == 1):
                groups[-1] += column
            elif column:
                groups.append(column)
        for group in groups:
            cycle(*group)
    return [(place(shape, one), place(shape, target[one])) for one in sorted(target)]


def load_body(scatter_ref, own_ref, columns_ref, rows_ref, sem):
    first = pltpu.make_async_copy(scatter_ref, columns_ref, sem.at[0])
    second = pltpu.make_async_copy(own_ref, rows_ref, sem.at[1])
    first.start()
    second.start()
    first.wait()
    second.wait()


def load(columns, own):
    vmem = pl.BlockSpec(memory_space=pltpu.VMEM)
    return pl.pallas_call(
        load_body,
        out_shape=[pltpu.VMEM(columns.shape, columns.dtype), pltpu.VMEM(own.shape, own.dtype)],
        in_specs=[pl.BlockSpec(memory_space=pltpu.HBM)] * 2,
        out_specs=[vmem] * 2,
        scratch_shapes=[pltpu.SemaphoreType.DMA((2,))],
        cost_estimate=pl.CostEstimate(flops=3 * 10**9, bytes_accessed=4 * columns.size, transcendentals=0),
        compiler_params=pltpu.CompilerParams(vmem_limit_bytes=1024 * 1024),
    )(pltpu.with_memory_space_constraint(columns, pltpu.HBM), pltpu.with_memory_space_constraint(own, pltpu.HBM))


def combine_body(own_ref, other_ref, source_ref):
    rows = own_ref.shape[0]
    mine = lax.axis_index(AXES[2]) * rows
    source_ref[pl.ds(pl.multiple_of(mine, rows), rows), :] = own_ref[...]
    source_ref[pl.ds(pl.multiple_of(rows - mine, rows), rows), :] = other_ref[...]


def combine(own, other):
    vmem = pl.BlockSpec(memory_space=pltpu.VMEM)
    arrays = [pltpu.with_memory_space_constraint(i, pltpu.VMEM) for i in (own, other)]
    return pl.pallas_call(
        combine_body,
        out_shape=pltpu.VMEM((2 * own.shape[0], own.shape[1]), own.dtype),
        in_specs=[vmem] * 2,
        out_specs=vmem,
        compiler_params=pltpu.CompilerParams(vmem_limit_bytes=1024 * 1024),
    )(*arrays)


def step_body(turn_in, west_ref, south_ref, source_ref, forward_ref, west_in, south_in, sent_ref, west_all, south_all, turn_ref, inflow):
    rows, modes = west_ref.shape
    a, b, row = (lax.axis_index(axis) for axis in AXES)

    turn = turn_in[0]
    turn_ref[0] = turn + 1

    @pl.when(jnp.logical_and(a + b == turn, row == 0))
    def _():
        @pl.loop(0, rows // 16)
        def _(i):
            part = pl.ds(pl.multiple_of(i * 16, 16), 16)
            west = jnp.where(a > 0, west_ref[part], 0)
            south = jnp.where(b > 0, south_ref[part], 0)
            west_all[part] = west
            south_all[part] = south
            inflow[part, :modes] = (source_ref[part, :modes].astype(jnp.float32) + west.astype(jnp.float32)).astype(jnp.bfloat16)
            inflow[part, modes:] = (source_ref[part, modes:].astype(jnp.float32) + south.astype(jnp.float32)).astype(jnp.bfloat16)

        sent_ref[...] = jnp.dot(inflow[...], forward_ref[...], preferred_element_type=jnp.float32).astype(jnp.bfloat16)


def step(turn, west, south, source, forward, west_all, south_all):
    rows, modes = west.shape
    vmem = pl.BlockSpec(memory_space=pltpu.VMEM)
    arrays = [pltpu.with_memory_space_constraint(i, pltpu.VMEM) for i in (west, south, source, forward, west_all, south_all)]
    face = pltpu.VMEM((rows, modes), jnp.bfloat16)
    smem = pl.BlockSpec(memory_space=pltpu.SMEM)
    sent, west_all, south_all, turn = pl.pallas_call(
        step_body,
        out_shape=[pltpu.VMEM((rows, 2 * modes), jnp.bfloat16), face, face, pltpu.SMEM((1,), jnp.int32)],
        in_specs=[smem] + [vmem] * 6,
        out_specs=[vmem] * 3 + [smem],
        scratch_shapes=[pltpu.VMEM((rows, 2 * modes), jnp.bfloat16)],
        input_output_aliases={5: 1, 6: 2},
        cost_estimate=pl.CostEstimate(flops=8 * rows * modes * modes, bytes_accessed=8 * modes * modes, transcendentals=0),
        compiler_params=pltpu.CompilerParams(vmem_limit_bytes=4 * 1024 * 1024),
    )(pltpu.with_memory_space_constraint(turn, pltpu.SMEM), *arrays)
    return sent[:, :modes], sent[:, modes:], west_all, south_all, turn


def keep_body(turn, west_ref, south_ref, west_all, south_all, faces_ref):
    modes = west_ref.shape[1]
    a, b, row = (lax.axis_index(axis) for axis in AXES)
    last = jnp.logical_and(a + b == turn, row == 0)
    for now, kept, part in ((west_ref, west_all, slice(0, modes)), (south_ref, south_all, slice(modes, 2 * modes))):

        @pl.when(last)
        def _():
            faces_ref[:, part] = now[...]

        @pl.when(jnp.logical_not(last))
        def _():
            faces_ref[:, part] = kept[...]


def keep(turn, west, south, west_all, south_all):
    vmem = pl.BlockSpec(memory_space=pltpu.VMEM)
    arrays = [pltpu.with_memory_space_constraint(i, pltpu.VMEM) for i in (west, south, west_all, south_all)]
    return pl.pallas_call(
        functools.partial(keep_body, turn),
        out_shape=pltpu.VMEM((west.shape[0], 2 * west.shape[1]), west.dtype),
        in_specs=[vmem] * 4,
        out_specs=vmem,
        compiler_params=pltpu.CompilerParams(vmem_limit_bytes=1024 * 1024),
    )(*arrays)


def reflect_body(faces_own, faces_got, source_ref, columns_ref, mine_ref, west_low, west_high, south_low, south_high, inflow):
    rows, width = faces_own.shape
    half, modes = rows // 2, width // 2
    row = lax.axis_index(AXES[2])

    @pl.when(row == 0)
    def _():
        mine_ref[...] = source_ref[:half].astype(jnp.float32) + faces_own[:half].astype(jnp.float32)

    @pl.when(row == 1)
    def _():
        @pl.loop(0, rows // 16)
        def _(i):
            part = pl.ds(pl.multiple_of(i * 16, 16), 16)
            inflow[part] = (source_ref[part].astype(jnp.float32) + faces_got[part].astype(jnp.float32)).astype(jnp.bfloat16)

        for k, (low, high) in enumerate(((west_low, west_high), (south_low, south_high))):
            back = jnp.dot(inflow[...], columns_ref[:, k * modes : (k + 1) * modes], preferred_element_type=jnp.float32).astype(jnp.bfloat16)
            low[...] = back[:half]
            high[...] = back[half:]
        mine_ref[...] = source_ref[half:].astype(jnp.float32) + faces_got[half:].astype(jnp.float32)


def reflect(*arrays):
    rows, modes = arrays[0].shape[0], arrays[0].shape[1] // 2
    vmem = pl.BlockSpec(memory_space=pltpu.VMEM)
    return pl.pallas_call(
        reflect_body,
        out_shape=[pltpu.VMEM((rows // 2, 2 * modes), jnp.float32)] + [pltpu.VMEM((rows // 2, modes), jnp.bfloat16)] * 4,
        in_specs=[vmem] * 4,
        out_specs=[vmem] * 5,
        scratch_shapes=[pltpu.VMEM((rows, 2 * modes), jnp.bfloat16)],
        cost_estimate=pl.CostEstimate(flops=8 * rows * modes * modes, bytes_accessed=8 * modes * modes, transcendentals=0),
        compiler_params=pltpu.CompilerParams(vmem_limit_bytes=4 * 1024 * 1024),
    )(*[pltpu.with_memory_space_constraint(i, pltpu.VMEM) for i in arrays])


def total_body(shape, mine_ref, west_low, west_high, south_low, south_high, out_ref):
    modes = west_low.shape[1]
    a, b, row = (lax.axis_index(axis) for axis in AXES)
    sides = ((west_low, west_high, slice(0, modes), a < shape[0] - 1), (south_low, south_high, slice(modes, 2 * modes), b < shape[1] - 1))
    for low, high, part, inside in sides:
        for k, ref in enumerate((low, high)):

            @pl.when(jnp.logical_and(row == k, inside))
            def _():
                out_ref[:, part] = mine_ref[:, part] + ref[...].astype(jnp.float32)

        @pl.when(jnp.logical_not(inside))
        def _():
            out_ref[:, part] = mine_ref[:, part]


def total(shape, *arrays):
    vmem = pl.BlockSpec(memory_space=pltpu.VMEM)
    return pl.pallas_call(
        functools.partial(total_body, shape),
        out_shape=jax.ShapeDtypeStruct(arrays[0].shape, jnp.float32),
        in_specs=[vmem] * 5,
        out_specs=vmem,
        compiler_params=pltpu.CompilerParams(vmem_limit_bytes=4 * 1024 * 1024),
    )(*[pltpu.with_memory_space_constraint(i, pltpu.VMEM) for i in arrays])


def back_moves(shape, west, high):
    nx, ny, _ = shape
    count = nx if west else ny
    target = {}
    for a in range(nx):
        for b in range(ny):
            k = a if west else b

            def at(step, row):
                return (a + step, b, row) if west else (a, b + step, row)

            if high:
                target[a, b, 1] = at(-1, 1) if k > 0 else at(0, 0)
                target[a, b, 0] = at(1, 0) if k < count - 1 else at(0, 1)
            else:
                mate = (a, b ^ 1) if west else (a ^ 1, b)
                target[a, b, 1] = at(-1, 0) if k > 0 else mate + (1,)
                target[a, b, 0] = at(1, 1) if k < count - 1 else mate + (0,)
    return [(place(shape, one), place(shape, target[one])) for one in sorted(target)]


def on_device(shape, sources, scatter):
    nx, ny, nr = shape
    own = sources[0, 0]
    columns = scatter[0, 0]
    rows, width = own.shape
    modes = width // 2
    cells = [(i, j, k) for i in range(nx) for j in range(ny) for k in range(nr)]
    across = [(place(shape, (i, j, k)), place(shape, (i, j, 1 - k))) for i, j, k in cells]
    other = lax.ppermute(own, AXES, across)
    columns, own = load(columns, own)
    source = combine(own, other)
    face = jnp.zeros((2 * rows, modes), jnp.bfloat16)
    east, north, west_all, south_all, turn = step(jnp.zeros((1,), jnp.int32), face, face, source, columns, face, face)
    for t in range(nx + ny - 2):
        west = lax.ppermute(east, AXES, step_moves(shape, t, True))
        south = lax.ppermute(north, AXES, step_moves(shape, t, False))
        if t < nx + ny - 3:
            east, north, west_all, south_all, turn = step(turn, west, south, source, columns, west_all, south_all)
    faces = keep(nx + ny - 2, west, south, west_all, south_all)
    mine, *parts = reflect(faces, lax.ppermute(faces, AXES, across[::2]), source, columns)
    returned = {}
    for k, west, high in ((0, True, False), (2, False, False), (1, True, True), (3, False, True)):
        returned[k] = lax.ppermute(parts[k], AXES, back_moves(shape, west, high))
    return total(shape, mine, *[returned[k] for k in range(4)])[None, None]


def solution(mesh):
    shape = tuple(mesh.shape[axis] for axis in AXES)
    placed = (P("gx", "gy", "row", None), P("gx", "gy", None, "row"))
    return jax.shard_map(
        functools.partial(on_device, shape), mesh=mesh, in_specs=placed, out_specs=P("gx", "gy", "row", None), check_vma=False
    )
```
